32 devices in a mesh: groups: 2 (over y), expert: 4 (over x, core), etp: 4 (over z).
Axes of the slice: x: 2, y: 2, z: 4, core: 2. Of those that a mesh axis runs over, the one named last changes fastest.
Arguments:
- tokens: bfloat16 [1024, 4096], P(('groups', 'expert'), 'etp'), parts along dimension 0, may hold values from -6 to 6
- route_ids: int32 [1024, 2], P(('groups', 'expert')), parts along dimension 0, may hold values from 0 to 3, all different within a row; in each aligned block of 128 rows (0 to 127, 128 to 255, ...) at most 96 rows name the same one
- gate_weights: float32 [1024, 2], P(('groups', 'expert')), parts along dimension 0, may hold values from 0.2 to 1
- w_gate: bfloat16 [4, 4096, 14336], P('expert', None, 'etp'), may hold values from -0.09375 to 0.09375
- w_up: bfloat16 [4, 4096, 14336], P('expert', None, 'etp'), may hold values from -0.09375 to 0.09375
- w_down: bfloat16 [4, 14336, 4096], P('expert', 'etp'), may hold values from -0.0625 to 0.0625
Outputs:
- mixed: bfloat16 [1024, 4096], P(('groups', 'expert'), 'etp'), parts along dimension 0
The draws below stay inside these ranges and needn't reach their ends.
There are 2 independent parts, one for each index of `groups`. The reference program is written for one: setup_inputs(seed, part) draws one part's arguments, and reference() takes and returns one part's arrays. A program takes and returns all parts, laid end to end along the dimension named above; an argument that names none is the same for every part. Nothing has to cross between parts.
Inputs may be any that keep to these rules, and one draw needn't show every extreme that they name: `route_ids`: each row names two different experts. In the rows of one index of expert (128 aligned rows), no expert is named by more than 96 rows, a bound that some block reaches.
All inputs are finite; a program needn't handle non-finite values.
Results may differ from the reference program's by a relative error of at most 0.024.
Values may be sent and summed in bfloat16 or wider, within the bound.
A program may use at most 192 MiB of HBM per device.

```python
import math
import jax
import jax.numpy as jnp
import numpy as np
from jax import lax

D = 4096
FF = 14336
TOK_DEV = 128
CAP = 96
EXPERTS = 4
TOKENS = 512
N_EXPERT = 4
N_ETP = 4


def spiked(drawn, key, source, target, parts, factor):
    owner, partner = [(jnp.arange(drawn.shape[dim]) // (drawn.shape[dim] // parts)).reshape([-1 if axis == dim else 1 for axis in range(drawn.ndim)]) for dim in (source, target)]
    chosen = jax.random.permutation(key, parts)[partner]
    strong = (owner == chosen) | (owner == (partner + parts // 2) % parts)
    return jnp.where(strong, factor * drawn, drawn)


def shard_levels(key, dims, pieces, smallest, largest):
    level = 1.0
    for dim, blocks in pieces:
        heights = jax.random.uniform(jax.random.fold_in(jax.random.fold_in(key, 6), dim), (blocks,), jnp.float32, smallest / len(pieces), largest / len(pieces))
        level = level * jnp.repeat(jnp.exp(heights), dims[dim] // blocks).reshape((-1,) + (1,) * (len(dims) - 1 - dim))
    return level


def shared_out(rng, own, number, rows, amount, top, limit, skew):
    ranking = jax.random.permutation(rng, amount)
    packed, ordinary = shares(amount, rows * top, limit, skew, True), shares(amount, rows * top, limit, skew, False)
    places = jnp.arange(amount)

    def named(sizes, offset_by):
        used = int((sizes > 0).sum())
        fixed = max(1, used // 4)
        passed = fixed + (places - fixed + offset_by * (used - fixed)) % max(1, amount - fixed)
        return jnp.zeros((amount,), jnp.int32).at[ranking[jnp.where(places < fixed, places, passed)]].set(jnp.asarray(sizes, jnp.int32))

    sizes = jnp.where(number % 4 == 0, named(packed, number // 4), named(ordinary, number - number // 4 - 1))
    mixed = jax.random.permutation(jax.random.fold_in(own, 3), amount)
    source_of, taker = mixed[0:amount // 2 * 2:2], mixed[1:amount // 2 * 2:2]
    room = jnp.minimum(sizes[source_of] - 1, limit - sizes[taker]) // 2
    room = jnp.where((source_of == ranking[0]) | (taker == ranking[0]) | (sizes[taker] == 0), 0, jnp.maximum(room, 0))
    passed = jax.random.randint(jax.random.fold_in(own, 4), (amount // 2,), 0, 1 << 20) % (room + 1)
    sizes = sizes.at[source_of].add(-passed).at[taker].add(passed)
    members = jnp.searchsorted(jnp.cumsum(sizes), jnp.arange(rows * top), side="right").astype(jnp.int32)
    table = members.reshape(top, rows).T
    table = table[jax.random.permutation(jax.random.fold_in(own, 1), rows)]
    offset_by = jax.random.randint(jax.random.fold_in(own, 2), (rows, 1), 0, top)
    return jnp.take_along_axis(table, (jnp.arange(top)[None, :] + offset_by) % top, axis=1)


def shares(number_of, total, reach, skew, full):
    portions = [(1 << 20) // math.isqrt(rank ** skew) + 1 for rank in range(1, number_of + 1)]
    largest = reach if full else min(reach, max(-(-total // number_of), total * portions[0] // sum(portions)))
    least = 1 if total - largest >= number_of - 1 else 0
    counts, spare = [largest] + [least] * (number_of - 1), total - largest - least * (number_of - 1)
    while spare > 0:
        movable = [i for i in range(1, number_of) if counts[i] < largest] or [i for i in range(1, number_of) if counts[i] < reach]
        pool, budget = sum([portions[i] for i in movable]), spare
        for i in movable:
            more = min(reach - counts[i], max(1, budget * portions[i] // pool), spare)
            counts[i] = counts[i] + more
            spare = spare - more
    return np.array(counts)


def noise(rng, dims, spread, limit, cuts=(), held_as=jnp.bfloat16):
    drawn = jax.random.normal(rng, dims, jnp.float32) * spread
    if len(cuts) > 0:
        drawn = shard_levels(rng, dims, cuts, -0.22, 0.18) * drawn
    return jnp.clip(drawn, min=-limit, max=limit).astype(held_as)


def bell_draw_with(key, extent, width, limit, shards, heavy, kind=jnp.bfloat16):
    result = width * jax.random.normal(key, extent, jnp.float32)
    if shards:
        result = result * shard_levels(key, extent, shards, -0.22, 0.18)
    return jnp.clip(spiked(result, jax.random.fold_in(key, 3), *heavy), -limit, limit).astype(kind)


def setup_inputs(seed: int = 0, part: int = 0) -> dict:
    streams_of = jax.random.split(jax.random.key(seed), 7)
    part_splits = jax.random.split(jax.random.fold_in(streams_of[6], part), 7)
    tokens = noise(part_splits[0], (TOKENS, D), 1.0, 6.0, ((0, 4), (1, 4)))
    route_ids_keys = jax.random.split(jax.random.fold_in(part_splits[1], 1), TOKENS // TOK_DEV)
    route_ids_turns = jax.random.permutation(jax.random.fold_in(part_splits[1], 3), TOKENS // TOK_DEV)
    route_ids = jax.vmap(lambda own, number: shared_out(jax.random.fold_in(part_splits[1], 2), own, number, TOK_DEV, EXPERTS, 2, CAP, 1))(route_ids_keys, route_ids_turns).reshape((TOKENS, 2))
    gate_weights = jnp.clip(0.2 + 0.8 * jax.random.uniform(part_splits[2], (TOKENS, 2), jnp.float32) ** shard_levels(part_splits[2], (TOKENS, 2), ((0, 4),), -0.2, 0.2), 0.2, 1.0)
    w_gate = noise(streams_of[3], (EXPERTS, D, FF), D ** -0.5, 0.09375, ((0, 4), (2, 4)))
    w_up = noise(streams_of[4], (EXPERTS, D, FF), D ** -0.5, 0.09375, ((0, 4), (2, 4)))
    w_down = bell_draw_with(streams_of[5], (EXPERTS, FF, D), FF ** -0.5, 0.0625, ((0, 4), (1, 4)), (1, 2, 4, 2.0))
    return {"tokens": tokens, "route_ids": route_ids, "gate_weights": gate_weights, "w_gate": w_gate, "w_up": w_up, "w_down": w_down}


def down_sum(hidden_wide, down_wide):
    group = FF // N_ETP
    rows = hidden_wide.shape[0]

    def add_group(index, total):
        start = (index * group).astype(jnp.int32)
        hidden_part = lax.dynamic_slice_in_dim(hidden_wide, start, group, 1)
        down_part = lax.dynamic_slice_in_dim(down_wide, start, group, 0)
        partial_value = jnp.dot(hidden_part, down_part, precision=lax.Precision.HIGHEST).astype(jnp.bfloat16)
        return total + partial_value.astype(jnp.float32)

    return lax.fori_loop(0, N_ETP, add_group, jnp.zeros((rows, D), jnp.float32))


def reference(tokens, route_ids, gate_weights, w_gate, w_up, w_down):
    slot_total = N_EXPERT * CAP
    summed = jnp.zeros((TOKENS, D), jnp.float32)
    token_block = (jnp.arange(TOKENS, dtype=jnp.int32) // TOK_DEV).astype(jnp.int32)
    for expert_number in range(EXPERTS):
        hit_mask = route_ids == expert_number
        routed = jnp.any(hit_mask, axis=1).astype(jnp.int32)
        weighting = jnp.sum(jnp.where(hit_mask, gate_weights, 0.0), axis=1)
        slot_index = (jnp.cumsum(routed.reshape(N_EXPERT, TOK_DEV), axis=1) - 1).reshape(TOKENS).astype(jnp.int32)
        target_row = jnp.where(routed == 1, token_block * CAP + slot_index, slot_total).astype(jnp.int32)
        buffer = jnp.zeros((slot_total, D), jnp.bfloat16).at[target_row].set(tokens, mode="drop")
        buffer_wide = buffer.astype(jnp.float32)
        gate_sum = jnp.dot(buffer_wide, w_gate[expert_number].astype(jnp.float32), precision=lax.Precision.HIGHEST)
        up_sum = jnp.dot(buffer_wide, w_up[expert_number].astype(jnp.float32), precision=lax.Precision.HIGHEST)
        hidden = (jax.nn.silu(gate_sum) * up_sum).astype(jnp.bfloat16)
        expert_out = down_sum(hidden.astype(jnp.float32), w_down[expert_number].astype(jnp.float32)).astype(jnp.bfloat16)
        picked = expert_out[jnp.minimum(target_row, slot_total - 1)]
        summed = summed + weighting[:, None] * picked.astype(jnp.float32)
    return summed.astype(jnp.bfloat16)
```

```python
import functools

import jax
import jax.numpy as jnp
from jax import lax
from jax.experimental import pallas as pl
from jax.experimental.pallas import tpu as pltpu
from jax.sharding import PartitionSpec as P

CAP = 96


def shards(tokens, route_ids, gate_weights, w_gate, w_up, w_down):
    cycle_size = lax.axis_size("expert")
    token_count, local_width = tokens.shape
    slot_total = cycle_size * CAP
    expert_iota = lax.broadcasted_iota(jnp.int32, (1, 1, cycle_size), 2)
    hit_mask = route_ids[:, :, None] == expert_iota
    routed = jnp.any(hit_mask, axis=1).astype(jnp.int32)
    weighting = jnp.sum(jnp.where(hit_mask, gate_weights[:, :, None], 0.0), axis=1)
    slot_index = jnp.cumsum(routed, axis=0) - 1
    expert_base = lax.broadcasted_iota(jnp.int32, (1, cycle_size), 1) * CAP
    target_slot = jnp.where(routed == 1, expert_base + slot_index, -1)
    slot_iota = lax.broadcasted_iota(jnp.int32, (1, 1, slot_total), 2)
    pick_table = target_slot[:, :, None] == slot_iota
    select_table = jnp.any(pick_table, axis=1).astype(jnp.bfloat16)
    combine_table = jnp.sum(jnp.where(pick_table, weighting[:, :, None], 0.0), axis=1)
    dispatched = jnp.dot(select_table.T, tokens, preferred_element_type=jnp.float32)
    dispatched = dispatched.astype(jnp.bfloat16).reshape(cycle_size, CAP, local_width)
    gate_local = w_gate[0]
    up_local = w_up[0]
    down_local = w_down[0]
    received = lax.all_to_all(dispatched, "expert", split_axis=0, concat_axis=0, tiled=True)
    columns_in = lax.all_gather(
        received.reshape(slot_total, local_width), "etp", axis=1, tiled=True
    )
    gate_sum = jnp.dot(columns_in, gate_local, preferred_element_type=jnp.float32)
    up_sum = jnp.dot(columns_in, up_local, preferred_element_type=jnp.float32)
    hidden = (jax.nn.silu(gate_sum) * up_sum).astype(jnp.bfloat16)
    partial_out = jnp.dot(hidden, down_local, preferred_element_type=jnp.float32).astype(
        jnp.bfloat16
    )
    finished = (
        lax.psum_scatter(partial_out, "etp", scatter_dimension=1, tiled=True)
        .astype(jnp.float32)
        .astype(jnp.bfloat16)
    )
    results = lax.all_to_all(
        finished.reshape(cycle_size, CAP, local_width),
        "expert",
        split_axis=0,
        concat_axis=0,
        tiled=True,
    )
    flat_results = results.reshape(slot_total, local_width).astype(jnp.float32)
    mixed = jnp.dot(combine_table, flat_results, precision=lax.Precision.HIGHEST)
    return mixed.astype(jnp.bfloat16)


FOUR = 4
HALVES = 2
RING_IN = 5
RING_OUT = 3
BLOCK = 256
LEAD = 4
TARGETS = (0, 0, 0, 1, 0, 1, 2, 1, 2, 1, 2, 2, 3, 3, 3, 3)


def partner(me, step):
    low = (me % 2 + step % 2) % 2
    high = (me // 2 + step // 2) % 2
    return low + 2 * high


def layer_kernel(
    tok_hbm, route_hbm, weight_hbm, gate_hbm, up_hbm, down_hbm, out_hbm,
    routes, weights, toks, chosen, pick, comb, acc_gate, acc_up, hidden,
    ring_in, ring_out, kept, core_out, core_in, x_out, x_in, z_out, z_in, out_vmem,
    sem_in, sem_out, sem_own, sem_put, meta_s, meta_r, z_s, z_r, zf_s,
    x_s, x_r, ca_s, ca_r, cb_s, cb_r, rc_s, rc_r, rx_s, rx_r, rz_s, rz_r,
):
    rows, width = tok_hbm.shape
    inner = gate_hbm.shape[2]
    e = lax.axis_index("expert")
    z = lax.axis_index("etp")
    middle = (z + 1) // 2 % 2
    sub = width // HALVES
    tile = inner // HALVES
    subs = FOUR * HALVES
    steps_in = subs * HALVES
    units = len(TARGETS)
    slabs = units // 2
    rank = [TARGETS[:i].count(TARGETS[i]) for i in range(units)]
    place = {(TARGETS[i], rank[i]): i for i in range(units)}

    def origin(p):
        return partner(z, p + middle * (p // 2) * (1 - 2 * (p % 2)))

    def fetch_in(t, slot):
        k = t // HALVES
        row = pl.multiple_of(origin(k // HALVES) * width + k % HALVES * sub, sub)
        col = pl.multiple_of(t % HALVES * tile, tile)
        return [
            pltpu.make_async_copy(
                hbm.at[0, pl.ds(row, sub), pl.ds(col, tile)],
                ring_in.at[slot, :, pl.ds(m * tile, tile)],
                sem_in.at[slot, m],
            )
            for m, hbm in enumerate((gate_hbm, up_hbm))
        ]

    def fetch_out(u):
        return [
            pltpu.make_async_copy(
                down_hbm.at[0, :, pl.ds(
                    pl.multiple_of(
                        partner(z, FOUR - 1 - TARGETS[i]) * width + rank[i] * BLOCK, BLOCK
                    ), BLOCK
                )],
                ring_out.at[u % RING_OUT, :, pl.ds(i % 2 * BLOCK, BLOCK)],
                sem_out.at[u % RING_OUT, i % 2],
            )
            for i in (2 * u, 2 * u + 1)
        ]

    def send(source, target, s_sem, r_sem, axis, step):
        me = e if axis == "expert" else z
        return pltpu.make_async_remote_copy(
            src_ref=source, dst_ref=target, send_sem=s_sem, recv_sem=r_sem,
            device_id={axis: partner(me, step)},
            device_id_type=pl.DeviceIdType.MESH,
        )

    barrier = pltpu.get_barrier_semaphore()

    def greet(axis, me, step):
        pl.semaphore_signal(
            barrier, inc=1, device_id={axis: partner(me, step)},
            device_id_type=pl.DeviceIdType.MESH,
        )

    greet("etp", z, 2)
    pl.when(middle == 1)(lambda: greet("etp", z, 3))
    greet("etp", z, 1)
    for step in (3, 2, 1):
        greet("expert", e, step)

    own = [
        pltpu.make_async_copy(route_hbm, routes.at[0], sem_own.at[0]),
        pltpu.make_async_copy(weight_hbm, weights.at[0], sem_own.at[1]),
    ] + [
        pltpu.make_async_copy(
            tok_hbm.at[:, pl.ds(h * sub, sub)], toks.at[0, 0, h], sem_own.at[2 + h]
        )
        for h in range(HALVES)
    ]
    for copy in own:
        copy.start()
    for copy in own:
        copy.wait()
    for t in range(RING_IN):
        for copy in fetch_in(t, t):
            copy.start()
    pl.semaphore_wait(barrier, FOUR + 1 + middle)

    meta_copies = [
        send(
            held.at[0], held.at[j], meta_s.at[m, j], meta_r.at[m, j], "expert", j,
        )
        for j in (2, 3, 1)
        for m, held in enumerate((routes, weights))
    ]
    near_copies = [
        send(toks.at[0, 0, h], toks.at[1, 0, h], z_s.at[0, h], z_r.at[1, h], "etp", 1)
        for h in range(HALVES)
    ]
    far_copies = [
        send(
            toks.at[0, 0, h], toks.at[3 - middle, 0, h], z_s.at[1, h],
            z_r.at[3 - middle, h], "etp", 2 + middle,
        )
        for h in range(HALVES)
    ]
    z_copies, forward, x_copies, ca_copies, cb_copies = [], [], [], [], []
    for k in range(subs):
        p, h = k // HALVES, k % HALVES
        mine = toks.at[p, 0, h]
        z_copies.append(send(mine, mine, zf_s.at[p, h], z_r.at[p, h], "etp", 1))
        x_copies.append(
            send(mine, toks.at[p, 2, h], x_s.at[k], x_r.at[k], "expert", 2)
        )
        ca_copies.append(
            send(mine, toks.at[p, 1, h], ca_s.at[k], ca_r.at[k], "expert", 1)
        )
        cb_copies.append(
            send(toks.at[p, 2, h], toks.at[p, 3, h], cb_s.at[k], cb_r.at[k], "expert", 1)
        )
    for copy in meta_copies:
        copy.start()
    for h in range(HALVES):
        x_copies[h].start()
        near_copies[h].start()
    for h in range(HALVES):
        far_copies[h].start()
        ca_copies[h].start()

    for copy in meta_copies:
        copy.wait_recv()
    earlier = (
        lax.broadcasted_iota(jnp.int32, (rows, rows), 0)
        < lax.broadcasted_iota(jnp.int32, (rows, rows), 1)
    ).astype(jnp.bfloat16)
    slot_row = lax.broadcasted_iota(jnp.int32, (rows, rows), 0).astype(jnp.float32)
    for j in range(FOUR):
        route, weigh = routes[j], weights[j]
        first = route[0:1, :] == e
        second = route[1:2, :] == e
        routed = jnp.where(first, 1.0, 0.0) + jnp.where(second, 1.0, 0.0)
        weight = jnp.where(first, weigh[0:1, :], 0.0) + jnp.where(second, weigh[1:2, :], 0.0)
        slot = jnp.dot(
            jnp.broadcast_to(routed, (16, rows)).astype(jnp.bfloat16), earlier,
            preferred_element_type=jnp.float32,
        )[0:1, :]
        slot = jnp.where(routed > 0.5, slot, -1.0)
        hit = slot_row == slot
        pick[j] = jnp.where(hit, 1.0, 0.0).astype(jnp.bfloat16)
        comb[j] = jnp.where(hit, weight, 0.0).T.astype(jnp.bfloat16)

    def pass_over(k):
        if k < subs:
            x_copies[k].wait_recv()
            cb_copies[k].start()

    def pass_on(k):
        if k < subs:
            if k < 2 * HALVES:
                z_copies[k].wait_recv()
            else:
                pl.when(middle == 0)(z_copies[k].wait_recv)
            x_copies[k].start()
            ca_copies[k].start()

    def pass_out(k):
        if k < subs:

            @pl.when(middle == 1)
            def _():
                z_copies[k].wait_recv()
                z_copies[k].start()

    def poll(k):
        pass_over(k)
        pass_on(k + HALVES)
        pass_out(k + 2 * HALVES)

    poll(0)
    for k in range(subs):
        p, h = k // HALVES, k % HALVES
        ca_copies[k].wait_recv()
        cb_copies[k].wait_recv()
        for j in range(FOUR):
            chosen[pl.ds(j * CAP, CAP), :] = jnp.dot(
                pick[j, 0:CAP, :], toks[p, j, h], preferred_element_type=jnp.float32
            ).astype(jnp.bfloat16)

        if k == subs - 1:
            for u in range(RING_OUT):
                for copy in fetch_out(u):
                    copy.start()

        def in_step(n, carry, k=k):
            if k + 1 < subs:
                pl.when(n == 1)(functools.partial(poll, k + 1))
            t = k * HALVES + n
            slot = lax.rem(t, RING_IN)
            for copy in fetch_in(t, slot):
                copy.wait()
            col = pl.ds(pl.multiple_of(n * tile, tile), tile)
            both = jnp.dot(chosen[...], ring_in[slot], preferred_element_type=jnp.float32)
            gate, up = both[:, :tile], both[:, tile:]
            if k > 0:
                gate = gate + acc_gate[:, col]
                up = up + acc_up[:, col]
            if k < subs - 1:
                acc_gate[:, col] = gate
                acc_up[:, col] = up
            else:
                hidden[:, col] = (gate / (1.0 + jnp.exp(-gate)) * up).astype(jnp.bfloat16)

            @pl.when(t + RING_IN < steps_in)
            def _():
                for copy in fetch_in(t + RING_IN, slot):
                    copy.start()

            return carry

        lax.fori_loop(0, HALVES, in_step, 0)

    core_copies = [
        send(
            core_out.at[pl.ds(2 * u, 2)], core_in.at[pl.ds(2 * u, 2)],
            rc_s.at[u], rc_r.at[u], "expert", 1,
        )
        for u in range(slabs)
    ]
    rx_copies = [
        send(x_out.at[i], x_in.at[i], rx_s.at[i], rx_r.at[i], "expert", 2)
        for i in range(units)
    ]
    rz_copies = [
        send(z_out.at[i], z_in.at[i], rz_s.at[i], rz_r.at[i], "etp", (1, 2, 1)[TARGETS[i]])
        for i in range(units) if TARGETS[i] < FOUR - 1
    ]
    outs = [
        pltpu.make_async_copy(
            out_vmem.at[q], out_hbm.at[:, pl.ds(q * BLOCK, BLOCK)], sem_put.at[q]
        )
        for q in range(width // BLOCK)
    ]

    def x_stage(u):
        core_copies[u].wait_recv()
        for i in (2 * u, 2 * u + 1):
            x_out[i] = (kept[i, 1] + core_in[i, 1].astype(jnp.float32)).astype(jnp.bfloat16)
            rx_copies[i].start()

    def z_stage(i):
        q = rank[i]
        adds = {1: (0,), 3: (2, 1)}.get(TARGETS[i], ())
        rx_copies[i].wait_recv()
        both = kept[i, 0] + core_in[i, 0].astype(jnp.float32) + x_in[i].astype(jnp.float32)
        for target in adds:
            rz_copies[place[target, q]].wait_recv()
            both = both + z_in[place[target, q]].astype(jnp.float32)
        if TARGETS[i] < FOUR - 1:
            z_out[i] = both.astype(jnp.bfloat16)
            rz_copies[i].start()
        else:
            out_vmem[q] = both.astype(jnp.bfloat16)
            outs[q].start()

    def down_slab(u):
        for copy in fetch_out(u):
            copy.wait()
        part = jnp.dot(
            hidden[...], ring_out[u % RING_OUT], preferred_element_type=jnp.float32
        ).astype(jnp.bfloat16)
        for j in range(FOUR):
            share = jnp.dot(
                comb[j, :, 0:CAP], part[j * CAP:(j + 1) * CAP, :],
                preferred_element_type=jnp.float32,
            )
            for m in range(2):
                piece = share[:, m * BLOCK:(m + 1) * BLOCK]
                if j % 2 == 0:
                    kept[2 * u + m, j // 2] = piece
                else:
                    core_out[2 * u + m, j // 2] = piece.astype(jnp.bfloat16)
        core_copies[u].start()
        if u + RING_OUT < slabs:
            for copy in fetch_out(u + RING_OUT):
                copy.start()

    late, sent = 0, 0
    for u in range(slabs):
        down_slab(u)
        while sent < u or sent == u < 2:
            x_stage(sent)
            sent += 1
        while 2 * sent - late > LEAD:
            z_stage(late)
            late += 1
    x_stage(slabs - 1)
    for i in range(late, units):
        z_stage(i)
    for copy in outs:
        copy.wait()

    @pl.when(middle == 1)
    def _():
        for copy in z_copies[2 * HALVES:]:
            copy.wait_send()

    for copy in (
        meta_copies + near_copies + far_copies + x_copies + ca_copies + cb_copies
        + core_copies + rx_copies + rz_copies
    ):
        copy.wait_send()


def fused(tokens, route_ids, gate_weights, w_gate, w_up, w_down):
    rows, width = tokens.shape
    inner = w_gate.shape[2]
    slots = FOUR * CAP
    units, subs = len(TARGETS), FOUR * HALVES
    bf, f32 = jnp.bfloat16, jnp.float32
    dma = pltpu.SemaphoreType.DMA
    hbm = pl.BlockSpec(memory_space=pl.ANY)
    return pl.pallas_call(
        layer_kernel,
        out_shape=jax.ShapeDtypeStruct((rows, width), bf),
        in_specs=[hbm] * 6,
        out_specs=hbm,
        scratch_shapes=[
            pltpu.VMEM((FOUR, 2, rows), jnp.int32),
            pltpu.VMEM((FOUR, 2, rows), f32),
            pltpu.VMEM((FOUR, FOUR, HALVES, rows, width // HALVES), bf),
            pltpu.VMEM((slots, width // HALVES), bf),
            pltpu.VMEM((FOUR, rows, rows), bf),
            pltpu.VMEM((FOUR, rows, rows), bf),
            pltpu.VMEM((slots, inner), f32),
            pltpu.VMEM((slots, inner), f32),
            pltpu.VMEM((slots, inner), bf),
            pltpu.VMEM((RING_IN, width // HALVES, inner), bf),
            pltpu.VMEM((RING_OUT, inner, 2 * BLOCK), bf),
            pltpu.VMEM((units, 2, rows, BLOCK), f32),
            pltpu.VMEM((units, 2, rows, BLOCK), bf),
            pltpu.VMEM((units, 2, rows, BLOCK), bf),
            pltpu.VMEM((units, rows, BLOCK), bf),
            pltpu.VMEM((units, rows, BLOCK), bf),
            pltpu.VMEM((units, rows, BLOCK), bf),
            pltpu.VMEM((units, rows, BLOCK), bf),
            pltpu.VMEM((width // BLOCK, rows, BLOCK), bf),
            dma((RING_IN, 2)), dma((RING_OUT, 2)), dma((2 + HALVES,)), dma((width // BLOCK,)),
            dma((2, FOUR)), dma((2, FOUR)),
            dma((2, HALVES)), dma((FOUR, HALVES)), dma((FOUR, HALVES)),
            dma((subs,)), dma((subs,)), dma((subs,)), dma((subs,)),
            dma((subs,)), dma((subs,)),
            dma((units // 2,)), dma((units // 2,)), dma((units,)), dma((units,)),
            dma((units,)), dma((units,)),
        ],
        compiler_params=pltpu.CompilerParams(
            collective_id=0, has_side_effects=True, vmem_limit_bytes=67043328
        ),
    )(tokens, route_ids.T, gate_weights.T, w_gate, w_up, w_down)


def pick_body(tokens, route_ids, gate_weights, w_gate, w_up, w_down):
    square = lax.axis_size("expert") == FOUR and lax.axis_size("etp") == FOUR
    whole = tokens.shape == (128, len(TARGETS) * BLOCK // FOUR)
    lanes = w_gate.shape[2] % (HALVES * 128) == 0
    body = fused if square and whole and lanes else shards
    return body(tokens, route_ids, gate_weights, w_gate, w_up, w_down)


def solution(mesh):
    return jax.shard_map(
        pick_body,
        mesh=mesh,
        in_specs=(
            P(("groups", "expert"), "etp"),
            P(("groups", "expert"), None),
            P(("groups", "expert"), None),
            P("expert", None, "etp"),
            P("expert", None, "etp"),
            P("expert", "etp", None),
        ),
        out_specs=P(("groups", "expert"), "etp"),
        check_vma=False,
    )
```

```python
import functools

import jax
import jax.numpy as jnp
from jax import lax
from jax.experimental import pallas as pl
from jax.experimental.pallas import tpu as pltpu
from jax.sharding import PartitionSpec as P

CAP = 96


def shards(tokens, route_ids, gate_weights, w_gate, w_up, w_down):
    cycle_size = lax.axis_size("expert")
    token_count, local_width = tokens.shape
    slot_total = cycle_size * CAP
    expert_iota = lax.broadcasted_iota(jnp.int32, (1, 1, cycle_size), 2)
    hit_mask = route_ids[:, :, None] == expert_iota
    routed = jnp.any(hit_mask, axis=1).astype(jnp.int32)
    weighting = jnp.sum(jnp.where(hit_mask, gate_weights[:, :, None], 0.0), axis=1)
    slot_index = jnp.cumsum(routed, axis=0) - 1
    expert_base = lax.broadcasted_iota(jnp.int32, (1, cycle_size), 1) * CAP
    target_slot = jnp.where(routed == 1, expert_base + slot_index, -1)
    slot_iota = lax.broadcasted_iota(jnp.int32, (1, 1, slot_total), 2)
    pick_table = target_slot[:, :, None] == slot_iota
    select_table = jnp.any(pick_table, axis=1).astype(jnp.bfloat16)
    combine_table = jnp.sum(jnp.where(pick_table, weighting[:, :, None], 0.0), axis=1)
    dispatched = jnp.dot(select_table.T, tokens, preferred_element_type=jnp.float32)
    dispatched = dispatched.astype(jnp.bfloat16).reshape(cycle_size, CAP, local_width)
    gate_local = w_gate[0]
    up_local = w_up[0]
    down_local = w_down[0]
    received = lax.all_to_all(dispatched, "expert", split_axis=0, concat_axis=0, tiled=True)
    columns_in = lax.all_gather(
        received.reshape(slot_total, local_width), "etp", axis=1, tiled=True
    )
    gate_sum = jnp.dot(columns_in, gate_local, preferred_element_type=jnp.float32)
    up_sum = jnp.dot(columns_in, up_local, preferred_element_type=jnp.float32)
    hidden = (jax.nn.silu(gate_sum) * up_sum).astype(jnp.bfloat16)
    partial_out = jnp.dot(hidden, down_local, preferred_element_type=jnp.float32).astype(
        jnp.bfloat16
    )
    finished = (
        lax.psum_scatter(partial_out, "etp", scatter_dimension=1, tiled=True)
        .astype(jnp.float32)
        .astype(jnp.bfloat16)
    )
    results = lax.all_to_all(
        finished.reshape(cycle_size, CAP, local_width),
        "expert",
        split_axis=0,
        concat_axis=0,
        tiled=True,
    )
    flat_results = results.reshape(slot_total, local_width).astype(jnp.float32)
    mixed = jnp.dot(combine_table, flat_results, precision=lax.Precision.HIGHEST)
    return mixed.astype(jnp.bfloat16)


FOUR = 4
HALVES = 2
RING_IN = 5
RING_OUT = 3
BLOCK = 256
EARLY = 2
WIDE = 4
READY = (0, 0, 1, 2, 3, 5, 6, 7)
RELAY = 3
TARGETS = (0, 1, 0, 1, 0, 1, 0, 1, 2, 2, 2, 2, 3, 3, 3, 3)


def partner(me, step):
    low = (me % 2 + step % 2) % 2
    high = (me // 2 + step // 2) % 2
    return low + 2 * high


def layer_kernel(
    tok_hbm, route_hbm, weight_hbm, gate_hbm, up_hbm, down_hbm, out_ref,
    routes, weights, toks, chosen, pick, comb, acc_gate, acc_up, hidden,
    ring_in, ring_out, kept, core_out, core_in, x_out, x_in, z_out, z_in,
    sem_in, sem_out, sem_own, sem_sent, meta_r, z_r, x_r, ca_r, cb_r, rc_r, rx_r, rz_r,
):
    rows, width = tok_hbm.shape
    inner = gate_hbm.shape[2]
    e = lax.axis_index("expert")
    z = lax.axis_index("etp")
    middle = (z + 1) // 2 % 2
    sub = width // HALVES
    tile = inner // HALVES
    subs = FOUR * HALVES
    steps_in = subs * HALVES
    units = len(TARGETS)
    slabs = units // 2
    rank = [TARGETS[:i].count(TARGETS[i]) for i in range(units)]
    place = {(TARGETS[i], rank[i]): i for i in range(units)}

    def origin(p):
        return partner(z, p + middle * (p // 2) * (1 - 2 * (p % 2)))

    def fetch_in(t, slot):
        k = t // HALVES
        row = pl.multiple_of(origin(k // HALVES) * width + k % HALVES * sub, sub)
        col = pl.multiple_of(t % HALVES * tile, tile)
        return [
            pltpu.make_async_copy(
                hbm.at[0, pl.ds(row, sub), pl.ds(col, tile)],
                ring_in.at[slot, :, pl.ds(m * tile, tile)],
                sem_in.at[slot],
            )
            for m, hbm in enumerate((gate_hbm, up_hbm))
        ]

    def await_in(slot):
        pltpu.make_async_copy(
            gate_hbm.at[0, pl.ds(0, sub), :], ring_in.at[slot], sem_in.at[slot]
        ).wait()

    def await_out(u):
        pltpu.make_async_copy(
            down_hbm.at[0, :, pl.ds(0, 2 * BLOCK)], ring_out.at[u % RING_OUT],
            sem_out.at[u % RING_OUT],
        ).wait()

    def step_of(target):
        return FOUR - 1 - target + middle * (target * (2 - target) * 2 - 1) * (target < 2)

    def fetch_out(u):
        return [
            pltpu.make_async_copy(
                down_hbm.at[0, :, pl.ds(
                    pl.multiple_of(
                        partner(z, step_of(TARGETS[i])) * width + rank[i] * BLOCK, BLOCK
                    ), BLOCK
                )],
                ring_out.at[u % RING_OUT, :, pl.ds(i % 2 * BLOCK, BLOCK)],
                sem_out.at[u % RING_OUT],
            )
            for i in (2 * u, 2 * u + 1)
        ]

    def send(source, target, kind, r_sem, axis, step):
        me = e if axis == "expert" else z
        return pltpu.make_async_remote_copy(
            src_ref=source, dst_ref=target, send_sem=sem_sent.at[kind], recv_sem=r_sem,
            device_id={axis: partner(me, step)},
            device_id_type=pl.DeviceIdType.MESH,
        )

    barrier = pltpu.get_barrier_semaphore()

    def greet(axis, me, step):
        pl.semaphore_signal(
            barrier, inc=1, device_id={axis: partner(me, step)},
            device_id_type=pl.DeviceIdType.MESH,
        )

    greet("etp", z, 2)
    pl.when(middle == 1)(lambda: greet("etp", z, 3))
    greet("etp", z, 1)
    for step in (3, 2, 1):
        greet("expert", e, step)

    own = [
        pltpu.make_async_copy(route_hbm, routes.at[0], sem_own.at[0]),
        pltpu.make_async_copy(weight_hbm, weights.at[0], sem_own.at[1]),
    ] + [
        pltpu.make_async_copy(
            tok_hbm.at[:, pl.ds(h * sub, sub)], toks.at[0, 0, h], sem_own.at[2 + h]
        )
        for h in range(HALVES)
    ]
    for copy in own:
        copy.start()
    for copy in own:
        copy.wait()
    for t in range(RING_IN):
        for copy in fetch_in(t, t):
            copy.start()

    earlier = (
        lax.broadcasted_iota(jnp.int32, (rows, rows), 0)
        < lax.broadcasted_iota(jnp.int32, (rows, rows), 1)
    ).astype(jnp.bfloat16)
    slot_row = lax.broadcasted_iota(jnp.int32, (rows, rows), 0).astype(jnp.float32)

    def place_block(j):
        route, weigh = routes[j], weights[j]
        first = route[0:1, :] == e
        second = route[1:2, :] == e
        routed = jnp.where(first, 1.0, 0.0) + jnp.where(second, 1.0, 0.0)
        weight = jnp.where(first, weigh[0:1, :], 0.0) + jnp.where(second, weigh[1:2, :], 0.0)
        slot = jnp.dot(
            jnp.broadcast_to(routed, (16, rows)).astype(jnp.bfloat16), earlier,
            preferred_element_type=jnp.float32,
        )[0:1, :]
        slot = jnp.where(routed > 0.5, slot, -1.0)
        hit = slot_row == slot
        pick[j] = jnp.where(hit, 1.0, 0.0).astype(jnp.bfloat16)
        comb[j] = jnp.where(hit, weight, 0.0).T.astype(jnp.bfloat16)

    place_block(0)
    pl.semaphore_wait(barrier, FOUR + 1 + middle)

    meta_copies = {
        j: [
            send(held.at[0], held.at[j], m, meta_r.at[m, j], "expert", j)
            for m, held in enumerate((routes, weights))
        ]
        for j in (2, 3, 1)
    }
    near_copies = [
        send(toks.at[0, 0, h], toks.at[1, 0, h], 2, z_r.at[1, h], "etp", 1)
        for h in range(HALVES)
    ]
    far_copies = [
        send(
            toks.at[0, 0, h], toks.at[3 - middle, 0, h], 2,
            z_r.at[3 - middle, h], "etp", 2 + middle,
        )
        for h in range(HALVES)
    ]
    z_copies, forward, x_copies, ca_copies, cb_copies = [], [], [], [], []
    for k in range(subs):
        p, h = k // HALVES, k % HALVES
        mine = toks.at[p, 0, h]
        z_copies.append(send(mine, mine, 3, z_r.at[p, h], "etp", 1))
        x_copies.append(
            send(mine, toks.at[p, 2, h], 4, x_r.at[k], "expert", 2)
        )
        ca_copies.append(
            send(mine, toks.at[p, 1, h], 5, ca_r.at[k], "expert", 1)
        )
        cb_copies.append(
            send(toks.at[p, 2, h], toks.at[p, 3, h], 6, cb_r.at[k], "expert", 1)
        )
    for pair in meta_copies.values():
        for copy in pair:
            copy.start()
    for h in range(HALVES):
        ca_copies[h].start()
        x_copies[h].start()
        near_copies[h].start()

    def send_far():
        for copy in far_copies:
            copy.start()

    pl.when(middle == 1)(send_far)

    def place_from(j):
        for copy in meta_copies[j]:
            copy.wait_recv()
        place_block(j)

    def pass_over(k):
        if k < subs:
            x_copies[k].wait_recv()
            cb_copies[k].start()

    def pass_on(k):
        if k < subs:
            if k < 2 * HALVES:
                z_copies[k].wait_recv()
            else:
                pl.when(middle == 0)(z_copies[k].wait_recv)
            x_copies[k].start()
            ca_copies[k].start()

    def pass_out(k):
        if k < subs:

            @pl.when(middle == 1)
            def _():
                z_copies[k].wait_recv()
                z_copies[k].start()

    def poll(k):
        pass_over(k)
        pass_out(k + 2 * HALVES)
        pass_on(k + HALVES)

    def select(k, first, stop):
        for j in range(first, stop):
            chosen[k % 2, pl.ds(j * CAP, CAP), :] = jnp.dot(
                pick[j, 0:CAP, :], toks[k // HALVES, j, k % HALVES],
                preferred_element_type=jnp.float32,
            ).astype(jnp.bfloat16)

    def multiply(k, first, stop, fresh, release):
        span = slice(first * CAP, stop * CAP)

        def tile_step(n):
            t = k * HALVES + n
            slot = lax.rem(t, RING_IN)
            start = n * tile
            col = pl.ds(start if isinstance(n, int) else pl.multiple_of(start, tile), tile)
            both = jnp.dot(
                chosen[k % 2, span, :], ring_in[slot], preferred_element_type=jnp.float32
            )
            gate, up = both[:, :tile], both[:, tile:]
            if k > 0:
                gate = gate + acc_gate[span, col]
                up = up + acc_up[span, col]
            if k < subs - 1:
                acc_gate[span, col] = gate
                acc_up[span, col] = up
            else:
                hidden[span, col] = (gate * (0.5 * jnp.tanh(0.5 * gate) + 0.5) * up).astype(jnp.bfloat16)

        def refill(n):
            t = k * HALVES + n
            slot = lax.rem(t, RING_IN)

            @pl.when(t + RING_IN < steps_in)
            def _():
                for copy in fetch_in(t + RING_IN, slot):
                    copy.start()

        def in_step(n, carry):
            if release and k + 1 < subs:
                pl.when(n == 1)(functools.partial(poll, k + 1))
            if fresh:
                await_in(lax.rem(k * HALVES + n, RING_IN))
            tile_step(n)
            if release:
                refill(n)
            return carry

        if k < WIDE:
            lax.fori_loop(0, HALVES, in_step, 0)
        else:
            if k + 1 < subs:
                poll(k + 1)
            for n in range(HALVES):
                await_in((k * HALVES + n) % RING_IN)
            for n in range(HALVES):
                tile_step(n)
            for n in range(HALVES):
                refill(n)

    place_from(1)
    for k in range(EARLY):
        ca_copies[k].wait_recv()
        select(k, 0, 2)
        multiply(k, 0, 2, True, False)
    place_from(2)
    place_from(3)
    poll(0)
    pl.when(middle == 0)(send_far)
    for k in range(EARLY):
        cb_copies[k].wait_recv()
        select(k, 2, FOUR)
        multiply(k, 2, FOUR, False, True)
    for k in range(EARLY, subs):
        ca_copies[k].wait_recv()
        cb_copies[k].wait_recv()
        select(k, 0, FOUR)
        if subs - 1 - k < RING_OUT:
            for copy in fetch_out(k - subs + RING_OUT):
                copy.start()
        multiply(k, 0, FOUR, True, True)

    core_copies = [
        [
            send(
                core_out.at[part, pl.ds(2 * u, 2)], core_in.at[part, pl.ds(2 * u, 2)],
                7, rc_r.at[part, u], "expert", 1,
            )
            for u in range(slabs)
        ]
        for part in range(2)
    ]
    rx_copies = [
        send(x_out.at[i], x_in.at[i], 8, rx_r.at[i], "expert", 2)
        for i in range(units)
    ]
    own_at = place[FOUR - 1, 0]
    rz_copies = []
    for i in range(own_at):
        target = TARGETS[i]
        at = i if target == 2 else i + middle * (own_at + rank[i] - i)
        step = 1 if target == 2 else 1 + middle * (1 + target)
        rz_copies.append(send(z_out.at[i], z_in.at[at], 9, rz_r.at[at], "etp", step))
    landings = [
        send(z_out.at[i], z_in.at[i], 9, rz_r.at[i], "etp", 1) for i in range(units)
    ]

    def x_stage(u):
        core_copies[1][u].wait_recv()
        for i in (2 * u, 2 * u + 1):
            x_out[i] = (kept[i, 1] + core_in[1, i].astype(jnp.float32)).astype(jnp.bfloat16)
            rx_copies[i].start()

    def z_sum(i):
        if i % 2 == 0:
            core_copies[0][i // 2].wait_recv()
        rx_copies[i].wait_recv()
        return kept[i, 0] + core_in[0, i].astype(jnp.float32) + x_in[i].astype(jnp.float32)

    def z_send(i):
        z_out[i] = z_sum(i).astype(jnp.bfloat16)
        rz_copies[i].start()

    def z_relay(i):
        both = z_sum(i)
        landings[i].wait_recv()
        z_out[i] = (both + z_in[i].astype(jnp.float32)).astype(jnp.bfloat16)
        rz_copies[i].start()

    def z_stage(i):
        if i < units:
            if TARGETS[i] < 2:
                pl.when(middle == 0)(functools.partial(z_send, i))
            elif TARGETS[i] == 2:
                z_send(i)
            else:
                both = z_sum(i)
                for at in (place[2, rank[i]], own_at + rank[i]):
                    landings[at].wait_recv()
                    both = both + z_in[at].astype(jnp.float32)
                col = rank[i] * BLOCK
                out_ref[:, col:col + BLOCK] = both.astype(jnp.bfloat16)
        if i >= RELAY and TARGETS[i - RELAY] < 2:
            pl.when(middle == 1)(functools.partial(z_relay, i - RELAY))

    def project(u, first, stop):
        part = jnp.dot(
            hidden[first * CAP:stop * CAP, :], ring_out[u % RING_OUT],
            preferred_element_type=jnp.float32,
        ).astype(jnp.bfloat16)
        for j in range(first, stop):
            share = jnp.dot(
                comb[j, :, 0:CAP], part[(j - first) * CAP:(j - first + 1) * CAP, :],
                preferred_element_type=jnp.float32,
            )
            for m in range(2):
                piece = share[:, m * BLOCK:(m + 1) * BLOCK]
                if j % 2 == 0:
                    kept[2 * u + m, j // 2] = piece
                else:
                    core_out[j // 2, 2 * u + m] = piece.astype(jnp.bfloat16)
        for half in range(stop // 2 - 1, first // 2 - 1, -1):
            core_copies[half][u].start()
        if first == 0 and u + RING_OUT < slabs:
            for copy in fetch_out(u + RING_OUT):
                copy.start()

    for u in range(EARLY):
        await_out(u)
        project(u, 2, FOUR)
    for u in range(EARLY):
        x_stage(u)
        project(u, 0, 2)
    done = 0
    for u in range(EARLY, slabs):
        await_out(u)
        project(u, 0, FOUR)
        if u > EARLY:
            x_stage(u - 1)
        for i in range(done, READY[u]):
            z_stage(i)
        done = READY[u]
    x_stage(slabs - 1)

    def drain(kind, source):
        send(source, source, kind, sem_sent.at[kind], "expert", 1).wait_send()

    drain(0, routes.at[pl.ds(0, FOUR - 1)])
    drain(1, weights.at[pl.ds(0, FOUR - 1)])
    drain(2, toks.at[0, pl.ds(0, 2)])
    pl.when(middle == 1)(lambda: drain(3, toks.at[0, pl.ds(0, 2)]))
    for kind in (4, 5, 6):
        drain(kind, toks.at[0])
    for i in range(done, units):
        z_stage(i)
    drain(7, core_out)
    drain(8, x_out)
    drain(9, z_out.at[pl.ds(0, own_at)])


def fused(tokens, route_ids, gate_weights, w_gate, w_up, w_down):
    rows, width = tokens.shape
    inner = w_gate.shape[2]
    slots = FOUR * CAP
    units, subs = len(TARGETS), FOUR * HALVES
    bf, f32 = jnp.bfloat16, jnp.float32
    dma = pltpu.SemaphoreType.DMA
    hbm = pl.BlockSpec(memory_space=pl.ANY)
    return pl.pallas_call(
        layer_kernel,
        out_shape=pltpu.VMEM((rows, width), bf),
        in_specs=[hbm] * 6,
        out_specs=pl.BlockSpec(memory_space=pltpu.VMEM),
        scratch_shapes=[
            pltpu.VMEM((FOUR, 2, rows), jnp.int32),
            pltpu.VMEM((FOUR, 2, rows), f32),
            pltpu.VMEM((FOUR, FOUR, HALVES, rows, width // HALVES), bf),
            pltpu.VMEM((2, slots, width // HALVES), bf),
            pltpu.VMEM((FOUR, rows, rows), bf),
            pltpu.VMEM((FOUR, rows, rows), bf),
            pltpu.VMEM((slots, inner), f32),
            pltpu.VMEM((slots, inner), f32),
            pltpu.VMEM((slots, inner), bf),
            pltpu.VMEM((RING_IN, width // HALVES, inner), bf),
            pltpu.VMEM((RING_OUT, inner, 2 * BLOCK), bf),
            pltpu.VMEM((units, 2, rows, BLOCK), f32),
            pltpu.VMEM((2, units, rows, BLOCK), bf),
            pltpu.VMEM((2, units, rows, BLOCK), bf),
            pltpu.VMEM((units, rows, BLOCK), bf),
            pltpu.VMEM((units, rows, BLOCK), bf),
            pltpu.VMEM((units, rows, BLOCK), bf),
            pltpu.VMEM((units, rows, BLOCK), bf),
            dma((RING_IN,)), dma((RING_OUT,)), dma((2 + HALVES,)), dma((10,)),
            dma((2, FOUR)), dma((FOUR, HALVES)), dma((subs,)), dma((subs,)), dma((subs,)),
            dma((2, units // 2)), dma((units,)), dma((units,)),
        ],
        compiler_params=pltpu.CompilerParams(
            collective_id=0, has_side_effects=True, vmem_limit_bytes=66500000
        ),
    )(tokens, route_ids.T, gate_weights.T, w_gate, w_up, w_down)


def pick_body(tokens, route_ids, gate_weights, w_gate, w_up, w_down):
    square = lax.axis_size("expert") == FOUR and lax.axis_size("etp") == FOUR
    whole = tokens.shape == (128, len(TARGETS) * BLOCK // FOUR)
    lanes = w_gate.shape[2] % (HALVES * 128) == 0
    body = fused if square and whole and lanes else shards
    return body(tokens, route_ids, gate_weights, w_gate, w_up, w_down)


def solution(mesh):
    return jax.shard_map(
        pick_body,
        mesh=mesh,
        in_specs=(
            P(("groups", "expert"), "etp"),
            P(("groups", "expert"), None),
            P(("groups", "expert"), None),
            P("expert", None, "etp"),
            P("expert", None, "etp"),
            P("expert", "etp", None),
        ),
        out_specs=P(("groups", "expert"), "etp"),
        check_vma=False,
    )
```
